32 devices in a mesh: gx: 4 (over y, core), gy: 4 (over z), gz: 2 (over x).
Axes of the slice: x: 2, y: 2, z: 4, core: 2. Of those that a mesh axis runs over, the one named last changes fastest.
Arguments:
- fluid_state: float32 [6, 32, 64, 256], P(None, 'gx', 'gy', 'gz'), may hold values from -1.6 to 140, as said below
Outputs:
- new_state: float32 [6, 32, 64, 256], P(None, 'gx', 'gy', 'gz')
The draws below stay inside these ranges and needn't reach their ends.
Inputs may be any that keep to these rules, and one draw needn't show every extreme that they name: `fluid_state`: each partial density is at least 0.05 times the density, the density lies between 0.5 and 2, and the pressure 0.4 (q5 - 0.5 times the sum over k = 0, 1, 2 of q(2+k)^2 / density) lies between 0.5 and 60.
All inputs are finite; a program needn't handle non-finite values.
Results may differ from the reference program's by a relative error of at most 0.0001.
Values sent between devices are 32-bit elements; how exact they have to be, the bound alone decides.
A program may use at most 64 MiB of HBM per device.

```python
import jax
import jax.numpy as jnp
from jax import lax

CX = 8
NX = 32
NY = 64
NZ = 256
N_GX = 4


def draw_fluid_state(key, part):
    subkeys = jax.random.split(key, 4)
    extent = (NX, NY, NZ)
    along_x = (jnp.arange(NX, dtype=jnp.float32) / NX)[:, None, None]
    density = jnp.exp(jax.random.uniform(subkeys[0], extent, jnp.float32, jnp.log(0.5), jnp.log(2.0)))
    colour = jax.random.uniform(subkeys[1], extent, jnp.float32, 0.05, 0.95)
    velocity = jax.random.uniform(subkeys[2], (3,) + extent, jnp.float32, -0.8, 0.8)
    pressure = 9.0 ** along_x * jnp.exp(jax.random.uniform(subkeys[3], extent, jnp.float32, jnp.log(0.5), jnp.log(2.0)))
    momentum = density * velocity
    energy = pressure / 0.4 + 0.5 * density * jnp.sum(velocity * velocity, axis=0)
    return jnp.concatenate([(colour * density)[None], ((1.0 - colour) * density)[None], momentum, energy[None]], axis=0).astype(jnp.float32)


def setup_inputs(seed: int = 0) -> dict:
    streams_of = jax.random.split(jax.random.key(seed), 2)
    return {
        "fluid_state": draw_fluid_state(jax.random.fold_in(streams_of[1], 71), 0),
    }


gamma_gas = 1.4
tension = 16.0
courant = 0.5
spacing = 0.5
weno_eps = 1e-06
normal_floor = 0.25

def primitives(conserved):
    density = conserved[0] + conserved[1]
    velocity = conserved[2:5] / density
    kinetic = 0.5 * lax.optimization_barrier(jnp.sum(conserved[2:5] * velocity, axis=0))
    pressure = (gamma_gas - 1.0) * (conserved[5] - kinetic)
    return (density, velocity, pressure)

def wave_speed(conserved):
    density, velocity, pressure = primitives(conserved)
    sound_speed = jnp.sqrt(gamma_gas * pressure / density)
    return lax.optimization_barrier(jnp.max(jnp.abs(velocity), axis=0)) + sound_speed

def trimmed(values, margin):
    for spatial in range(3):
        axis_pos = values.ndim - 3 + spatial
        values = lax.slice_in_dim(values, margin, values.shape[axis_pos] - margin, axis=axis_pos)
    return values

def keep_core(values, which_axis):
    for spatial in range(3):
        if spatial != which_axis:
            axis_pos = values.ndim - 3 + spatial
            values = lax.slice_in_dim(values, 3, values.shape[axis_pos] - 3, axis=axis_pos)
    return values

def derivative(source, which_axis):
    forward = source
    backward = source
    for spatial in range(3):
        axis_pos = source.ndim - 3 + spatial
        extent = source.shape[axis_pos]
        if spatial == which_axis:
            forward = lax.slice_in_dim(forward, 2, extent, axis=axis_pos)
            backward = lax.slice_in_dim(backward, 0, extent - 2, axis=axis_pos)
        else:
            forward = lax.slice_in_dim(forward, 1, extent - 1, axis=axis_pos)
            backward = lax.slice_in_dim(backward, 1, extent - 1, axis=axis_pos)
    return (forward - backward) / (2.0 * spacing)

def colour_of(conserved):
    return conserved[0] / (conserved[0] + conserved[1])

def gradient_of(colour):
    return jnp.stack([derivative(colour, 0), derivative(colour, 1), derivative(colour, 2)])

def unit_normals(gradient):
    length = jnp.sqrt(lax.optimization_barrier(jnp.sum(gradient * gradient, axis=0)))
    return gradient / jnp.maximum(length, normal_floor)

def curvature_of(normals):
    return -(derivative(normals[0], 0) + derivative(normals[1], 1) + derivative(normals[2], 2))

def weno_face(minus_two, minus_one, middle, plus_one, plus_two):
    stencil_a = (2.0 * minus_two - 7.0 * minus_one + 11.0 * middle) / 6.0
    stencil_b = (-minus_one + 5.0 * middle + 2.0 * plus_one) / 6.0
    stencil_c = (2.0 * middle + 5.0 * plus_one - plus_two) / 6.0
    smooth_a = 13.0 / 12.0 * (minus_two - 2.0 * minus_one + middle) ** 2 + 0.25 * (minus_two - 4.0 * minus_one + 3.0 * middle) ** 2
    smooth_b = 13.0 / 12.0 * (minus_one - 2.0 * middle + plus_one) ** 2 + 0.25 * (minus_one - plus_one) ** 2
    smooth_c = 13.0 / 12.0 * (middle - 2.0 * plus_one + plus_two) ** 2 + 0.25 * (3.0 * middle - 4.0 * plus_one + plus_two) ** 2
    weight_a = 0.1 / (weno_eps + smooth_a) ** 2
    weight_b = 0.6 / (weno_eps + smooth_b) ** 2
    weight_c = 0.3 / (weno_eps + smooth_c) ** 2
    return (weight_a * stencil_a + weight_b * stencil_b + weight_c * stencil_c) / (weight_a + weight_b + weight_c)

def flux_tendency(padded, top_speed):
    interior_shape = (6, padded.shape[1] - 6, padded.shape[2] - 6, padded.shape[3] - 6)
    tendency = jnp.zeros(interior_shape, jnp.float32)
    for which_axis in range(3):
        axis_pos = 1 + which_axis
        conserved = keep_core(padded, which_axis)
        density, velocity, pressure = primitives(conserved)
        normal_speed = velocity[which_axis]
        momenta = []
        for spatial in range(3):
            moving = conserved[2 + spatial] * normal_speed
            if spatial == which_axis:
                moving = moving + pressure
            momenta.append(moving)
        flux_whole = jnp.stack([conserved[0] * normal_speed, conserved[1] * normal_speed, momenta[0], momenta[1], momenta[2], (conserved[5] + pressure) * normal_speed])
        plus_part = 0.5 * (flux_whole + top_speed * conserved)
        minus_part = 0.5 * (flux_whole - top_speed * conserved)
        face_count = plus_part.shape[axis_pos] - 5

        def shifted(values, offset):
            return lax.slice_in_dim(values, 2 + offset, 2 + offset + face_count, axis=axis_pos)
        face_flux = weno_face(shifted(plus_part, -2), shifted(plus_part, -1), shifted(plus_part, 0), shifted(plus_part, 1), shifted(plus_part, 2))
        face_flux = face_flux + weno_face(shifted(minus_part, 3), shifted(minus_part, 2), shifted(minus_part, 1), shifted(minus_part, 0), shifted(minus_part, -1))
        upper_face = lax.slice_in_dim(face_flux, 1, face_count, axis=axis_pos)
        lower_face = lax.slice_in_dim(face_flux, 0, face_count - 1, axis=axis_pos)
        tendency = tendency - (upper_face - lower_face) / spacing
    return tendency

def capillary(interior, gradient, curvature):
    velocity = interior[2:5] / (interior[0] + interior[1])
    capillary_force = tension * curvature * gradient
    capillary_work = lax.optimization_barrier(jnp.sum(capillary_force * velocity, axis=0))
    zero_rows = jnp.zeros((2,) + curvature.shape, jnp.float32)
    return jnp.concatenate([zero_rows, capillary_force, capillary_work[None]], axis=0)

def section_block(slab_block, top_speed):
    colour_wide = colour_of(trimmed(slab_block, 1))
    gradient_wide = gradient_of(colour_wide)
    curvature = curvature_of(unit_normals(gradient_wide))
    gradient = trimmed(gradient_wide, 1)
    interior = trimmed(slab_block, 3)
    timestep = courant * spacing / (3.0 * top_speed)
    tendency = flux_tendency(slab_block, top_speed) + capillary(interior, gradient, curvature)
    return interior + timestep * tendency

def reference(fluid_state):
    top_speed = jnp.max(wave_speed(fluid_state))
    padded = jnp.pad(fluid_state, ((0, 0), (3, 3), (3, 3), (3, 3)), mode='wrap')

    def one_slab(slab_index):
        slab_start = slab_index * CX
        slab_block = lax.dynamic_slice_in_dim(padded, slab_start, CX + 6, axis=1)
        return section_block(slab_block, top_speed)
    all_slabs = lax.map(one_slab, jnp.arange(N_GX, dtype=jnp.int32))
    return jnp.moveaxis(all_slabs, 0, 1).reshape(6, NX, NY, NZ)
```

```python
import functools

import jax
import jax.numpy as jnp
from jax import lax
from jax.experimental import pallas as pl
from jax.experimental.pallas import tpu as pltpu
from jax.sharding import PartitionSpec as P

gamma_gas = 1.4
tension = 16.0
courant = 0.5
spacing = 0.5
weno_eps = 1e-06
normal_floor = 0.25

MESH = pl.DeviceIdType.MESH
SUB, LANES = 8, 128
SCALE = 0.25
F32 = jnp.float32


def primitives(q):
    inverse = 1.0 / (q[0] + q[1])
    u = [q[2 + k] * inverse for k in range(3)]
    kinetic = 0.5 * (q[2] * u[0] + q[3] * u[1] + q[4] * u[2])
    return inverse, u, (gamma_gas - 1.0) * (q[5] - kinetic)


def scaled_flux(q, k):
    _, u, p = primitives(q)
    speed = (0.5 * SCALE) * u[k]
    out = [q[c] * speed for c in range(5)] + [(q[5] + p) * speed]
    out[2 + k] = out[2 + k] + (0.5 * SCALE) * p
    return out


def correction(e0, e1, e2, third_a, third_b):
    q0, q1, q2 = e0 * e0, e1 * e1, e2 * e2
    a = q1 * q2
    b = 3.0 * (q0 * q1)
    total = a + (b + 6.0 * (q0 * q2))
    return (a * third_a + b * third_b) / total


def differences(v):
    n = len(v)
    d = [v[i + 1] - v[i] for i in range(n - 1)]
    h = [None] + [0.5 * (d[i] - d[i - 1]) for i in range(1, n - 1)]
    e = [None] + [h[i] * h[i] * (13.0 / 3.0) + weno_eps * SCALE * SCALE for i in range(1, n - 1)]
    j = [None, None] + [(2.0 / 3.0) * (h[i] - h[i - 1]) for i in range(2, n - 1)]
    return d, h, e, j


def square(value):
    return value * value


def weno_tendency(flux, state):
    n = len(flux)
    vp = [f + s for f, s in zip(flux, state)]
    vm = [f - s for f, s in zip(flux, state)]
    d, h, e, j = differences(vp)
    dm, hm, em, jm = differences(vm)
    faces = []
    for i in range(2, n - 3):
        fix = correction(
            e[i - 1] + square(d[i - 1] + h[i - 1]),
            e[i] + square(d[i - 1] + h[i]),
            e[i + 1] + square(h[i + 1] - d[i]),
            j[i],
            0.5 * j[i + 1],
        )
        fix_m = correction(
            em[i + 2] + square(hm[i + 2] - dm[i + 1]),
            em[i + 1] + square(hm[i + 1] - dm[i + 1]),
            em[i] + square(hm[i] + dm[i]),
            jm[i + 2],
            0.5 * jm[i + 1],
        )
        linear = (vp[i] + vm[i + 1]) + 0.5 * (d[i - 1] - dm[i + 1]) + (2.0 / 3.0) * (h[i] + hm[i + 1])
        faces.append(linear + (fix_m - fix))
    return [faces[i + 1] - faces[i] for i in range(len(faces) - 1)]


def kernel(sizes, q_hbm, out_ref, px, py, pz, fx, fy, fz, tq, zsend, zleft, zright, ts0, ts1, tsa, tsb, speed_ref,
           gb, nb, tb, nxp, nyp, nzp, nzsend, nzleft, nzright, src, ay, tz,
           local_sem, send_sem, recv_sem, sa_sem, ra_sem, sb_sem, rb_sem):
    ngx, ngy, ngz = sizes
    X, Y, Z = px.shape[1] - 6, px.shape[2], px.shape[3]
    step = Z // SUB
    lines = X * Y
    ix, iy, iz = lax.axis_index("gx"), lax.axis_index("gy"), lax.axis_index("gz")
    offsets_b = [(a, b) for a in range(ngy) for b in range(ngz) if (a, b) != (0, 0)]

    load = pltpu.make_async_copy(q_hbm, px.at[:, 3 : 3 + X], local_sem)
    load.start()
    barrier = pltpu.get_barrier_semaphore()

    def peer_x(offset):
        return {"gx": lax.rem(ix + offset + ngx, ngx)}

    def peer_yz(a, b):
        return {"gy": lax.rem(iy + a + ngy, ngy), "gz": lax.rem(iz + b + ngz, ngz)}

    for offset in range(1, ngx):
        pl.semaphore_signal(barrier, inc=1, device_id=peer_x(offset), device_id_type=MESH)
    for a, b in offsets_b:
        pl.semaphore_signal(barrier, inc=1, device_id=peer_yz(a, b), device_id_type=MESH)

    row = lax.broadcasted_iota(jnp.int32, (SUB, LANES), 0)
    pxf = px.reshape(6 * (X + 6) * Y, LANES)
    tqf = tq.reshape(6 * Z, lines)
    halves = Y // SUB

    def rows_y(base, y):
        return pl.ds(base + y, SUB, stride=Y)

    def rows_z(base, b):
        return pl.ds(base + b, SUB, stride=step)

    load.wait()
    best = None
    for x in range(X):
        for half in range(halves):
            q = [px[c, 3 + x, half * SUB : (half + 1) * SUB, :] for c in range(6)]
            inverse, u, p = primitives(q)
            top = jnp.maximum(jnp.maximum(jnp.abs(u[0]), jnp.abs(u[1])), jnp.abs(u[2]))
            top = top + jnp.sqrt(gamma_gas * p * inverse)
            best = top if best is None else jnp.maximum(best, top)
    ts0[...] = best

    def lay_out(c, carry):
        for y in range(Y):
            py[c, 3 + y] = pxf[rows_y((c * (X + 6) + 3) * Y, y), :]
        turned = px[c, 3 : 3 + X].reshape(lines, Z).T
        tq[c] = turned
        zsend[c] = jnp.where(row < 4, turned[:SUB], turned[Z - SUB :])
        return carry

    lax.fori_loop(0, 6, lay_out, 0)
    pl.semaphore_wait(barrier, ngx - 1 + len(offsets_b))

    def remote(source, target, index, peer, sends=send_sem, recvs=recv_sem):
        copy = pltpu.make_async_remote_copy(
            src_ref=source, dst_ref=target, send_sem=sends.at[index], recv_sem=recvs.at[index],
            device_id=peer, device_id_type=MESH,
        )
        copy.start()
        return copy

    reduce_a = [remote(ts0, tsa.at[o - 1], o - 1, peer_x(o), sa_sem, ra_sem) for o in range(1, ngx)]
    xlow, xhigh, ilow, ihigh = pl.ds(0, 3), pl.ds(3 + X, 3), pl.ds(3, 3), pl.ds(X, 3)
    first, rest = pl.ds(0, 2), pl.ds(2, 4)
    halo_x0 = [
        remote(px.at[first, ihigh], px.at[first, xlow], 0, peer_x(1)),
        remote(px.at[first, ilow], px.at[first, xhigh], 1, peer_x(-1)),
    ]
    halo_z = [remote(zsend, zleft, 2, peer_yz(0, 1))]
    if ngz > 2:
        halo_z.append(remote(zsend, zright, 3, peer_yz(0, -1)))
        from_right = zright
    else:
        from_right = zleft
    halo_y = [
        remote(py.at[:, pl.ds(Y, 3)], py.at[:, pl.ds(0, 3)], 4, peer_yz(1, 0)),
        remote(py.at[:, pl.ds(3, 3)], py.at[:, pl.ds(3 + Y, 3)], 5, peer_yz(-1, 0)),
    ]
    halo_x1 = [
        remote(px.at[rest, ihigh], px.at[rest, xlow], 6, peer_x(1)),
        remote(px.at[rest, ilow], px.at[rest, xhigh], 7, peer_x(-1)),
    ]

    def fill_z(c, carry):
        for b in range(step):
            pz[c, 3 + b] = tqf[rows_z(c * Z, b), :]
        return carry

    lax.fori_loop(0, 6, fill_z, 0)

    def flux_x(at):
        for half in range(halves):
            part = pl.ds(half * SUB, SUB)
            values = scaled_flux([px[c, at, part, :] for c in range(6)], 0)
            for c in range(6):
                fx[c, at, part, :] = values[c]

    def flux_of(padded, target, k, at):
        values = scaled_flux([padded[c, at] for c in range(6)], k)
        for c in range(6):
            target[c, at] = values[c]

    def inner_x(t, carry):
        flux_x(3 + 2 * t)
        flux_x(4 + 2 * t)
        return carry

    def inner_yz(t, carry):
        for extra in range(2):
            flux_of(py, fy, 1, 3 + 2 * t + extra)
            flux_of(pz, fz, 2, 3 + 2 * t + extra)
        return carry

    lax.fori_loop(0, X // 2, inner_x, 0)

    for copy in reduce_a:
        copy.wait()
    best = ts0[...]
    for o in range(ngx - 1):
        best = jnp.maximum(best, tsa[o])
    ts1[...] = best

    lax.fori_loop(0, Y // 2, inner_yz, 0)
    reduce_b = [
        remote(ts1, tsb.at[o], o, peer_yz(*offsets_b[o]), sb_sem, rb_sem) for o in range(len(offsets_b))
    ]

    def colour(q0, q1):
        return q0 / (q0 + q1)

    central = 1.0 / (2.0 * spacing)
    for copy in halo_z:
        copy.wait()

    def join_z(c, carry):
        for s in range(3):
            low = pltpu.roll(pz[c, step + s], 1, 0)
            left = jnp.broadcast_to(zleft[c, pl.ds(5 + s, 1), :], (SUB, LANES))
            pz[c, s] = jnp.where(row == 0, left, low)
            high = pltpu.roll(pz[c, 3 + s], SUB - 1, 0)
            right = jnp.broadcast_to(from_right[c, pl.ds(s, 1), :], (SUB, LANES))
            pz[c, 3 + step + s] = jnp.where(row == SUB - 1, right, high)
        return carry

    lax.fori_loop(0, 6, join_z, 0)
    colours = [colour(pz[0, 2 + b], pz[1, 2 + b]) for b in range(step + 2)]
    for b in range(step):
        tb[rows_z(0, b), :] = (colours[b + 2] - colours[b]) * central
    gb[2] = tb[...].T
    for s in range(3):
        flux_of(pz, fz, 2, s)
        flux_of(pz, fz, 2, 3 + step + s)

    for copy in halo_y:
        copy.wait()
    colours = [colour(py[0, 2 + y], py[1, 2 + y]) for y in range(Y + 2)]
    gbf = gb.reshape(3 * lines, LANES)
    for y in range(Y):
        gbf[rows_y(lines, y), :] = (colours[y + 2] - colours[y]) * central

    for copy in halo_x0:
        copy.wait()
    for half in range(halves):
        part = pl.ds(half * SUB, SUB)
        colours = [colour(px[0, 2 + x, part, :], px[1, 2 + x, part, :]) for x in range(X + 2)]
        for x in range(X):
            at = pl.ds(x * Y + half * SUB, SUB)
            g = [(colours[x + 2] - colours[x]) * central, gb[1, at, :], gb[2, at, :]]
            gb[0, at, :] = g[0]
            length = jnp.sqrt(g[0] * g[0] + g[1] * g[1] + g[2] * g[2])
            inverse = 1.0 / jnp.maximum(length, normal_floor)
            nxp[1 + x, part, :] = g[0] * inverse
            nb[0, at, :] = g[1] * inverse
            nb[1, at, :] = g[2] * inverse
    nbf = nb.reshape(2 * lines, LANES)
    tb[...] = nb[1].T
    nzsend[...] = jnp.where(row < 4, tb[:SUB, :], tb[Z - SUB :, :])
    for y in range(Y):
        nyp[1 + y] = nbf[rows_y(0, y), :]
    for b in range(step):
        nzp[1 + b] = tb[rows_z(0, b), :]
    normals = [
        remote(nxp.at[pl.ds(X, 1)], nxp.at[pl.ds(0, 1)], 8, peer_x(1)),
        remote(nxp.at[pl.ds(1, 1)], nxp.at[pl.ds(1 + X, 1)], 9, peer_x(-1)),
        remote(nyp.at[pl.ds(Y, 1)], nyp.at[pl.ds(0, 1)], 10, peer_yz(1, 0)),
        remote(nyp.at[pl.ds(1, 1)], nyp.at[pl.ds(1 + Y, 1)], 11, peer_yz(-1, 0)),
        remote(nzsend, nzleft, 12, peer_yz(0, 1)),
    ]
    if ngz > 2:
        normals.append(remote(nzsend, nzright, 13, peer_yz(0, -1)))
        normal_right = nzright
    else:
        normal_right = nzleft
    for s in range(3):
        flux_of(py, fy, 1, s)
        flux_of(py, fy, 1, 3 + Y + s)

    for copy in reduce_b:
        copy.wait()
    best = ts1[...]
    for o in range(len(offsets_b)):
        best = jnp.maximum(best, tsb[o])
    best = jnp.max(jnp.max(best, axis=1, keepdims=True), axis=0, keepdims=True)
    speed_ref[...] = jnp.broadcast_to(best, (SUB, LANES))

    def sweep_z(c, carry):
        scaled = (0.5 * SCALE) * speed_ref[...]
        count = step + 6
        parts = weno_tendency([fz[c, s] for s in range(count)], [pz[c, s] * scaled for s in range(count)])
        tzf = tz.reshape(6 * Z, lines)
        for b in range(step):
            tzf[rows_z(c * Z, b), :] = parts[b]
        return carry

    def sweep_y(c, carry):
        scaled = (0.5 * SCALE) * speed_ref[...]
        count = Y + 6
        parts = weno_tendency([fy[c, s] for s in range(count)], [py[c, s] * scaled for s in range(count)])
        ayf = ay.reshape(6 * lines, LANES)
        for y in range(Y):
            ayf[rows_y(c * lines, y), :] = parts[y]
        return carry

    lax.fori_loop(0, 6, sweep_z, 0)
    lax.fori_loop(0, 6, sweep_y, 0)

    for copy in normals:
        copy.wait()
    left = jnp.broadcast_to(nzleft[pl.ds(SUB - 1, 1), :], (SUB, LANES))
    nzp[0] = jnp.where(row == 0, left, pltpu.roll(nzp[step], 1, 0))
    right = jnp.broadcast_to(normal_right[pl.ds(0, 1), :], (SUB, LANES))
    nzp[1 + step] = jnp.where(row == SUB - 1, right, pltpu.roll(nzp[1], SUB - 1, 0))
    for b in range(step):
        tb[rows_z(0, b), :] = nzp[b + 2] - nzp[b]
    nb[1] = tb[...].T
    for y in range(Y):
        nbf[rows_y(0, y), :] = nyp[y + 2] - nyp[y]
    zero = jnp.zeros((SUB, LANES), F32)
    for x in range(X):
        for half in range(halves):
            part = pl.ds(half * SUB, SUB)
            at = pl.ds(x * Y + half * SUB, SUB)
            q = [px[c, 3 + x, part, :] for c in range(5)]
            inverse = 1.0 / (q[0] + q[1])
            along = (nxp[x + 2, part, :] - nxp[x, part, :]) + nb[0, at, :] + nb[1, at, :]
            pull = (-tension * central) * along
            force = [pull * gb[k, at, :] for k in range(3)]
            src[0, at, :] = zero
            src[1, at, :] = zero
            for k in range(3):
                src[2 + k, at, :] = force[k]
            src[5, at, :] = (force[0] * q[2] + force[1] * q[3] + force[2] * q[4]) * inverse

    for copy in halo_x1:
        copy.wait()
    for s in range(3):
        flux_x(s)
        flux_x(3 + X + s)

    def sweep_x(c, carry):
        top = speed_ref[...]
        scaled = (0.5 * SCALE) * top
        timestep = (courant * spacing) / (3.0 * top)
        slope = timestep * (-1.0 / (spacing * SCALE))
        count = X + 6
        back = tz[c].T
        for half in range(halves):
            part = pl.ds(half * SUB, SUB)
            state = [px[c, s, part, :] for s in range(count)]
            parts = weno_tendency([fx[c, s, part, :] for s in range(count)], [v * scaled for v in state])
            for x in range(X):
                start = x * Y + half * SUB
                at = pl.ds(start, SUB)
                change = parts[x] + ay[c, at, :] + back[start : start + SUB]
                out_ref[c, x, part, :] = state[3 + x] + (slope * change + timestep * src[c, at, :])
        return carry

    lax.fori_loop(0, 6, sweep_x, 0)


def solution(mesh):
    sizes = tuple(mesh.shape[name] for name in ("gx", "gy", "gz"))
    others = sizes[1] * sizes[2] - 1

    def per_device(q):
        _, X, Y, Z = q.shape
        step = Z // SUB
        lines = X * Y
        assert X == SUB and Y % SUB == 0 and Z == LANES and lines == LANES and min(sizes) > 1

        def vmem(*shape):
            return pltpu.VMEM(shape, F32)

        dma = pltpu.SemaphoreType.DMA
        return pl.pallas_call(
            functools.partial(kernel, sizes),
            name="section",
            out_shape=jax.ShapeDtypeStruct(q.shape, F32),
            in_specs=[pl.BlockSpec(memory_space=pl.ANY)],
            out_specs=pl.BlockSpec(memory_space=pltpu.VMEM),
            scratch_shapes=[
                vmem(6, X + 6, Y, Z), vmem(6, Y + 6, X, Z), vmem(6, step + 6, SUB, lines),
                vmem(6, X + 6, Y, Z), vmem(6, Y + 6, X, Z), vmem(6, step + 6, SUB, lines),
                vmem(6, Z, lines), vmem(6, SUB, lines), vmem(6, SUB, lines), vmem(6, SUB, lines),
                vmem(SUB, LANES), vmem(SUB, LANES), vmem(sizes[0] - 1, SUB, LANES), vmem(others, SUB, LANES),
                vmem(SUB, LANES),
                vmem(3, lines, Z), vmem(2, lines, Z), vmem(Z, lines),
                vmem(X + 2, Y, Z), vmem(Y + 2, X, Z), vmem(step + 2, SUB, lines),
                vmem(SUB, lines), vmem(SUB, lines), vmem(SUB, lines),
                vmem(6, lines, Z), vmem(6, lines, Z), vmem(6, Z, lines),
                dma, dma((14,)), dma((14,)),
                dma((sizes[0] - 1,)), dma((sizes[0] - 1,)), dma((others,)), dma((others,)),
            ],
            compiler_params=pltpu.CompilerParams(collective_id=0, has_side_effects=True),
        )(q)

    placed = P(None, "gx", "gy", "gz")
    return jax.shard_map(per_device, mesh=mesh, in_specs=(placed,), out_specs=placed, check_vma=False)
```

```python
import functools

import jax
import jax.numpy as jnp
from jax import lax
from jax.experimental import pallas as pl
from jax.experimental.pallas import tpu as pltpu
from jax.sharding import PartitionSpec as P

gamma_gas = 1.4
tension = 16.0
courant = 0.5
spacing = 0.5
weno_eps = 1e-06
normal_floor = 0.25

MESH = pl.DeviceIdType.MESH
SUB, LANES = 8, 128
SCALE = 0.25
F32 = jnp.float32


def primitives(q):
    inverse = 1.0 / (q[0] + q[1])
    u = [q[2 + k] * inverse for k in range(3)]
    kinetic = 0.5 * (q[2] * u[0] + q[3] * u[1] + q[4] * u[2])
    return inverse, u, (gamma_gas - 1.0) * (q[5] - kinetic)


def scaled_flux(q, k):
    _, u, p = primitives(q)
    speed = (0.5 * SCALE) * u[k]
    out = [q[c] * speed for c in range(5)] + [(q[5] + p) * speed]
    out[2 + k] = out[2 + k] + (0.5 * SCALE) * p
    return out


def correction(e0, e1, e2, third_a, third_b):
    q0, q1, q2 = e0 * e0, e1 * e1, e2 * e2
    a = q1 * q2
    b = 3.0 * (q0 * q1)
    total = a + (b + 6.0 * (q0 * q2))
    return (a * third_a + b * third_b) / total


def differences(v):
    n = len(v)
    d = [v[i + 1] - v[i] for i in range(n - 1)]
    h = [None] + [0.5 * (d[i] - d[i - 1]) for i in range(1, n - 1)]
    e = [None] + [h[i] * h[i] * (13.0 / 3.0) + weno_eps * SCALE * SCALE for i in range(1, n - 1)]
    j = [None, None] + [(2.0 / 3.0) * (h[i] - h[i - 1]) for i in range(2, n - 1)]
    return d, h, e, j


def square(value):
    return value * value


def weno_tendency(flux, state):
    n = len(flux)
    vp = [f + s for f, s in zip(flux, state)]
    vm = [f - s for f, s in zip(flux, state)]
    d, h, e, j = differences(vp)
    dm, hm, em, jm = differences(vm)
    faces = []
    for i in range(2, n - 3):
        fix = correction(
            e[i - 1] + square(d[i - 1] + h[i - 1]),
            e[i] + square(d[i - 1] + h[i]),
            e[i + 1] + square(h[i + 1] - d[i]),
            j[i],
            0.5 * j[i + 1],
        )
        fix_m = correction(
            em[i + 2] + square(hm[i + 2] - dm[i + 1]),
            em[i + 1] + square(hm[i + 1] - dm[i + 1]),
            em[i] + square(hm[i] + dm[i]),
            jm[i + 2],
            0.5 * jm[i + 1],
        )
        linear = (vp[i] + vm[i + 1]) + 0.5 * (d[i - 1] - dm[i + 1]) + (2.0 / 3.0) * (h[i] + hm[i + 1])
        faces.append(linear + (fix_m - fix))
    return [faces[i + 1] - faces[i] for i in range(len(faces) - 1)]


def rounds(sizes):
    x, y, z = sizes
    plane = [(0, a, b) for a in range(y) for b in range(z)][1:]
    line = [(a, 0, 0) for a in range(1, x)]
    if x * y * z > 64:
        return line, plane
    return [(a, b, c) for a in range(x) for b in range(y) for c in range(z)][1:], []


def kernel(sizes, q_hbm, out_ref, px, py, pz, fx, fy, fz, tq, zsend, zleft, zright, ts0, ts1, tsa, tsb, speed_ref,
           gb, nb, tb, nxp, nyp, nzp, nzsend, nzleft, nzright, src, ay, tz,
           local_sem, send_sem, recv_sem, sa_sem, ra_sem, sb_sem, rb_sem):
    ngx, ngy, ngz = sizes
    X, Y, Z = px.shape[1] - 6, px.shape[2], px.shape[3]
    step = Z // SUB
    lines = X * Y
    ix, iy, iz = lax.axis_index("gx"), lax.axis_index("gy"), lax.axis_index("gz")
    offsets_a, offsets_b = rounds(sizes)

    load = pltpu.make_async_copy(q_hbm, px.at[:, 3 : 3 + X], local_sem)
    load.start()
    barrier = pltpu.get_barrier_semaphore()

    def peer_x(offset):
        return {"gx": lax.rem(ix + offset + ngx, ngx)}

    def peer_yz(a, b):
        return {"gy": lax.rem(iy + a + ngy, ngy), "gz": lax.rem(iz + b + ngz, ngz)}

    def peer(offset):
        return {**peer_x(offset[0]), **peer_yz(offset[1], offset[2])}

    for offset in offsets_a + offsets_b:
        pl.semaphore_signal(barrier, inc=1, device_id=peer(offset), device_id_type=MESH)

    row = lax.broadcasted_iota(jnp.int32, (SUB, LANES), 0)
    pxf = px.reshape(6 * (X + 6) * Y, LANES)
    tqf = tq.reshape(6 * Z, lines)
    halves = Y // SUB

    def rows_y(base, y):
        return pl.ds(base + y, SUB, stride=Y)

    def rows_z(base, b):
        return pl.ds(base + b, SUB, stride=step)

    load.wait()
    best = None
    for x in range(X):
        for half in range(halves):
            q = [px[c, 3 + x, half * SUB : (half + 1) * SUB, :] for c in range(6)]
            inverse, u, p = primitives(q)
            top = jnp.maximum(jnp.maximum(jnp.abs(u[0]), jnp.abs(u[1])), jnp.abs(u[2]))
            top = top + jnp.sqrt(gamma_gas * p * inverse)
            best = top if best is None else jnp.maximum(best, top)
    ts0[...] = jnp.max(best, axis=0, keepdims=True)
    pl.semaphore_wait(barrier, len(offsets_a) + len(offsets_b))

    def remote(source, target, index, peer, sends=send_sem, recvs=recv_sem):
        copy = pltpu.make_async_remote_copy(
            src_ref=source, dst_ref=target, send_sem=sends.at[index], recv_sem=recvs.at[index],
            device_id=peer, device_id_type=MESH,
        )
        copy.start()
        return copy

    reduce_a = [remote(ts0, tsa.at[o], o, peer(offset), sa_sem, ra_sem) for o, offset in enumerate(offsets_a)]
    xlow, xhigh, ilow, ihigh = pl.ds(0, 3), pl.ds(3 + X, 3), pl.ds(3, 3), pl.ds(X, 3)
    first, rest = pl.ds(0, 2), pl.ds(2, 4)
    halo_x0 = [
        remote(px.at[first, ihigh], px.at[first, xlow], 0, peer_x(1)),
        remote(px.at[first, ilow], px.at[first, xhigh], 1, peer_x(-1)),
    ]
    halo_x1 = [
        remote(px.at[rest, ihigh], px.at[rest, xlow], 6, peer_x(1)),
        remote(px.at[rest, ilow], px.at[rest, xhigh], 7, peer_x(-1)),
    ]

    def lay_out(c, carry):
        for y in range(Y):
            py[c, 3 + y] = pxf[rows_y((c * (X + 6) + 3) * Y, y), :]
        turned = px[c, 3 : 3 + X].reshape(lines, Z).T
        tq[c] = turned
        zsend[c] = jnp.where(row < 4, turned[:SUB], turned[Z - SUB :])
        return carry

    lax.fori_loop(0, 6, lay_out, 0)
    halo_z = [remote(zsend, zleft, 2, peer_yz(0, 1))]
    if ngz > 2:
        halo_z.append(remote(zsend, zright, 3, peer_yz(0, -1)))
        from_right = zright
    else:
        from_right = zleft
    halo_y = [
        remote(py.at[:, pl.ds(Y, 3)], py.at[:, pl.ds(0, 3)], 4, peer_yz(1, 0)),
        remote(py.at[:, pl.ds(3, 3)], py.at[:, pl.ds(3 + Y, 3)], 5, peer_yz(-1, 0)),
    ]

    def fill_z(c, carry):
        for b in range(step):
            pz[c, 3 + b] = tqf[rows_z(c * Z, b), :]
        return carry

    lax.fori_loop(0, 6, fill_z, 0)

    def flux_x(at):
        for half in range(halves):
            part = pl.ds(half * SUB, SUB)
            values = scaled_flux([px[c, at, part, :] for c in range(6)], 0)
            for c in range(6):
                fx[c, at, part, :] = values[c]

    def flux_of(padded, target, k, at):
        values = scaled_flux([padded[c, at] for c in range(6)], k)
        for c in range(6):
            target[c, at] = values[c]

    def inner_x(t, carry):
        flux_x(3 + 2 * t)
        flux_x(4 + 2 * t)
        return carry

    def inner_yz(t, carry):
        for extra in range(2):
            flux_of(py, fy, 1, 3 + 2 * t + extra)
            flux_of(pz, fz, 2, 3 + 2 * t + extra)
        return carry

    lax.fori_loop(0, X // 2, inner_x, 0)

    lax.fori_loop(0, Y // 2, inner_yz, 0)
    reduce_b = []
    if offsets_b:
        for copy in reduce_a:
            copy.wait()
        ts1[...] = jnp.maximum(ts0[...], jnp.max(tsa[...], axis=0))
        reduce_b = [remote(ts1, tsb.at[o], o, peer(offset), sb_sem, rb_sem) for o, offset in enumerate(offsets_b)]

    def colour(q0, q1):
        return q0 / (q0 + q1)

    central = 1.0 / (2.0 * spacing)
    for copy in halo_z:
        copy.wait()

    def join_z(c, carry):
        for s in range(3):
            low = pltpu.roll(pz[c, step + s], 1, 0)
            left = jnp.broadcast_to(zleft[c, pl.ds(5 + s, 1), :], (SUB, LANES))
            pz[c, s] = jnp.where(row == 0, left, low)
            high = pltpu.roll(pz[c, 3 + s], SUB - 1, 0)
            right = jnp.broadcast_to(from_right[c, pl.ds(s, 1), :], (SUB, LANES))
            pz[c, 3 + step + s] = jnp.where(row == SUB - 1, right, high)
        return carry

    lax.fori_loop(0, 6, join_z, 0)
    colours = [colour(pz[0, 2 + b], pz[1, 2 + b]) for b in range(step + 2)]
    for b in range(step):
        tb[rows_z(0, b), :] = (colours[b + 2] - colours[b]) * central
    gb[2] = tb[...].T
    for s in range(3):
        flux_of(pz, fz, 2, s)
        flux_of(pz, fz, 2, 3 + step + s)

    for copy in halo_y:
        copy.wait()
    colours = [colour(py[0, 2 + y], py[1, 2 + y]) for y in range(Y + 2)]
    gbf = gb.reshape(3 * lines, LANES)
    for y in range(Y):
        gbf[rows_y(lines, y), :] = (colours[y + 2] - colours[y]) * central

    for copy in halo_x0:
        copy.wait()
    for half in range(halves):
        part = pl.ds(half * SUB, SUB)
        colours = [colour(px[0, 2 + x, part, :], px[1, 2 + x, part, :]) for x in range(X + 2)]
        for x in range(X):
            at = pl.ds(x * Y + half * SUB, SUB)
            g = [(colours[x + 2] - colours[x]) * central, gb[1, at, :], gb[2, at, :]]
            gb[0, at, :] = g[0]
            length = jnp.sqrt(g[0] * g[0] + g[1] * g[1] + g[2] * g[2])
            inverse = 1.0 / jnp.maximum(length, normal_floor)
            nxp[1 + x, part, :] = g[0] * inverse
            nb[0, at, :] = g[1] * inverse
            nb[1, at, :] = g[2] * inverse
    nbf = nb.reshape(2 * lines, LANES)
    tb[...] = nb[1].T
    nzsend[...] = jnp.where(row < 4, tb[:SUB, :], tb[Z - SUB :, :])
    for y in range(Y):
        nyp[1 + y] = nbf[rows_y(0, y), :]
    for b in range(step):
        nzp[1 + b] = tb[rows_z(0, b), :]
    normals = [
        remote(nxp.at[pl.ds(X, 1)], nxp.at[pl.ds(0, 1)], 8, peer_x(1)),
        remote(nxp.at[pl.ds(1, 1)], nxp.at[pl.ds(1 + X, 1)], 9, peer_x(-1)),
        remote(nyp.at[pl.ds(Y, 1)], nyp.at[pl.ds(0, 1)], 10, peer_yz(1, 0)),
        remote(nyp.at[pl.ds(1, 1)], nyp.at[pl.ds(1 + Y, 1)], 11, peer_yz(-1, 0)),
        remote(nzsend, nzleft, 12, peer_yz(0, 1)),
    ]
    if ngz > 2:
        normals.append(remote(nzsend, nzright, 13, peer_yz(0, -1)))
        normal_right = nzright
    else:
        normal_right = nzleft
    for s in range(3):
        flux_of(py, fy, 1, s)
        flux_of(py, fy, 1, 3 + Y + s)

    for copy in reduce_b if offsets_b else reduce_a:
        copy.wait()
    mine, others = (ts1, tsb) if offsets_b else (ts0, tsa)
    best = jnp.max(jnp.maximum(mine[...], jnp.max(others[...], axis=0)), axis=1, keepdims=True)
    speed_ref[...] = jnp.broadcast_to(best, (SUB, LANES))

    def sweep_z(c, carry):
        scaled = (0.5 * SCALE) * speed_ref[...]
        count = step + 6
        parts = weno_tendency([fz[c, s] for s in range(count)], [pz[c, s] * scaled for s in range(count)])
        tzf = tz.reshape(6 * Z, lines)
        for b in range(step):
            tzf[rows_z(c * Z, b), :] = parts[b]
        return carry

    def sweep_y(c, carry):
        scaled = (0.5 * SCALE) * speed_ref[...]
        count = Y + 6
        parts = weno_tendency([fy[c, s] for s in range(count)], [py[c, s] * scaled for s in range(count)])
        ayf = ay.reshape(6 * lines, LANES)
        for y in range(Y):
            ayf[rows_y(c * lines, y), :] = parts[y]
        return carry

    lax.fori_loop(0, 6, sweep_z, 0)
    lax.fori_loop(0, 6, sweep_y, 0)

    for copy in normals:
        copy.wait()
    left = jnp.broadcast_to(nzleft[pl.ds(SUB - 1, 1), :], (SUB, LANES))
    nzp[0] = jnp.where(row == 0, left, pltpu.roll(nzp[step], 1, 0))
    right = jnp.broadcast_to(normal_right[pl.ds(0, 1), :], (SUB, LANES))
    nzp[1 + step] = jnp.where(row == SUB - 1, right, pltpu.roll(nzp[1], SUB - 1, 0))
    for b in range(step):
        tb[rows_z(0, b), :] = nzp[b + 2] - nzp[b]
    nb[1] = tb[...].T
    for y in range(Y):
        nbf[rows_y(0, y), :] = nyp[y + 2] - nyp[y]
    zero = jnp.zeros((SUB, LANES), F32)
    for x in range(X):
        for half in range(halves):
            part = pl.ds(half * SUB, SUB)
            at = pl.ds(x * Y + half * SUB, SUB)
            q = [px[c, 3 + x, part, :] for c in range(5)]
            inverse = 1.0 / (q[0] + q[1])
            along = (nxp[x + 2, part, :] - nxp[x, part, :]) + nb[0, at, :] + nb[1, at, :]
            pull = (-tension * central) * along
            force = [pull * gb[k, at, :] for k in range(3)]
            src[0, at, :] = zero
            src[1, at, :] = zero
            for k in range(3):
                src[2 + k, at, :] = force[k]
            src[5, at, :] = (force[0] * q[2] + force[1] * q[3] + force[2] * q[4]) * inverse

    for copy in halo_x1:
        copy.wait()
    for s in range(3):
        flux_x(s)
        flux_x(3 + X + s)

    def sweep_x(c, carry):
        top = speed_ref[...]
        scaled = (0.5 * SCALE) * top
        timestep = (courant * spacing) / (3.0 * top)
        slope = timestep * (-1.0 / (spacing * SCALE))
        count = X + 6
        back = tz[c].T
        for half in range(halves):
            part = pl.ds(half * SUB, SUB)
            state = [px[c, s, part, :] for s in range(count)]
            parts = weno_tendency([fx[c, s, part, :] for s in range(count)], [v * scaled for v in state])
            for x in range(X):
                start = x * Y + half * SUB
                at = pl.ds(start, SUB)
                change = parts[x] + ay[c, at, :] + back[start : start + SUB]
                out_ref[c, x, part, :] = state[3 + x] + (slope * change + timestep * src[c, at, :])
        return carry

    lax.fori_loop(0, 6, sweep_x, 0)


def solution(mesh):
    sizes = tuple(mesh.shape[name] for name in ("gx", "gy", "gz"))
    count_a, count_b = (max(len(offsets), 1) for offsets in rounds(sizes))

    def per_device(q):
        _, X, Y, Z = q.shape
        step = Z // SUB
        lines = X * Y
        assert X == SUB and Y % SUB == 0 and Z == LANES and lines == LANES and min(sizes) > 1

        def vmem(*shape):
            return pltpu.VMEM(shape, F32)

        dma = pltpu.SemaphoreType.DMA
        return pl.pallas_call(
            functools.partial(kernel, sizes),
            name="section",
            out_shape=pltpu.VMEM(q.shape, F32),
            in_specs=[pl.BlockSpec(memory_space=pltpu.HBM)],
            out_specs=pl.BlockSpec(memory_space=pltpu.VMEM),
            scratch_shapes=[
                vmem(6, X + 6, Y, Z), vmem(6, Y + 6, X, Z), vmem(6, step + 6, SUB, lines),
                vmem(6, X + 6, Y, Z), vmem(6, Y + 6, X, Z), vmem(6, step + 6, SUB, lines),
                vmem(6, Z, lines), vmem(6, SUB, lines), vmem(6, SUB, lines), vmem(6, SUB, lines),
                vmem(1, LANES), vmem(1, LANES), vmem(count_a, 1, LANES), vmem(count_b, 1, LANES),
                vmem(SUB, LANES),
                vmem(3, lines, Z), vmem(2, lines, Z), vmem(Z, lines),
                vmem(X + 2, Y, Z), vmem(Y + 2, X, Z), vmem(step + 2, SUB, lines),
                vmem(SUB, lines), vmem(SUB, lines), vmem(SUB, lines),
                vmem(6, lines, Z), vmem(6, lines, Z), vmem(6, Z, lines),
                dma, dma((14,)), dma((14,)),
                dma((count_a,)), dma((count_a,)), dma((count_b,)), dma((count_b,)),
            ],
            compiler_params=pltpu.CompilerParams(collective_id=0, has_side_effects=True, vmem_limit_bytes=24 * 2**20),
        )(pltpu.with_memory_space_constraint(q, pltpu.HBM))

    placed = P(None, "gx", "gy", "gz")
    return jax.shard_map(per_device, mesh=mesh, in_specs=(placed,), out_specs=placed, check_vma=False)
```

```python
import functools

import jax
import jax.numpy as jnp
from jax import lax
from jax.experimental import pallas as pl
from jax.experimental.pallas import tpu as pltpu
from jax.sharding import PartitionSpec as P

gamma_gas = 1.4
tension = 16.0
courant = 0.5
spacing = 0.5
weno_eps = 1e-06
normal_floor = 0.25

MESH = pl.DeviceIdType.MESH
SUB, LANES = 8, 128
SCALE = 0.25
F32 = jnp.float32


def primitives(q):
    inverse = 1.0 / (q[0] + q[1])
    u = [q[2 + k] * inverse for k in range(3)]
    kinetic = 0.5 * (q[2] * u[0] + q[3] * u[1] + q[4] * u[2])
    return inverse, u, (gamma_gas - 1.0) * (q[5] - kinetic)


def scaled_flux(q, k):
    _, u, p = primitives(q)
    speed = (0.5 * SCALE) * u[k]
    out = [q[c] * speed for c in range(5)] + [(q[5] + p) * speed]
    out[2 + k] = out[2 + k] + (0.5 * SCALE) * p
    return out


def correction(e0, e1, e2, third_a, third_b):
    q0, q1, q2 = e0 * e0, e1 * e1, e2 * e2
    a = q1 * q2
    b = 3.0 * (q0 * q1)
    total = a + (b + 6.0 * (q0 * q2))
    return (a * third_a + b * third_b) / total


def differences(v):
    n = len(v)
    d = [v[i + 1] - v[i] for i in range(n - 1)]
    h = [None] + [0.5 * (d[i] - d[i - 1]) for i in range(1, n - 1)]
    e = [None] + [h[i] * h[i] * (13.0 / 3.0) + weno_eps * SCALE * SCALE for i in range(1, n - 1)]
    j = [None, None] + [(2.0 / 3.0) * (h[i] - h[i - 1]) for i in range(2, n - 1)]
    return d, h, e, j


def square(value):
    return value * value


def weno_tendency(flux, state):
    n = len(flux)
    vp = [f + s for f, s in zip(flux, state)]
    vm = [f - s for f, s in zip(flux, state)]
    d, h, e, j = differences(vp)
    dm, hm, em, jm = differences(vm)
    faces = []
    for i in range(2, n - 3):
        fix = correction(
            e[i - 1] + square(d[i - 1] + h[i - 1]),
            e[i] + square(d[i - 1] + h[i]),
            e[i + 1] + square(h[i + 1] - d[i]),
            j[i],
            0.5 * j[i + 1],
        )
        fix_m = correction(
            em[i + 2] + square(hm[i + 2] - dm[i + 1]),
            em[i + 1] + square(hm[i + 1] - dm[i + 1]),
            em[i] + square(hm[i] + dm[i]),
            jm[i + 2],
            0.5 * jm[i + 1],
        )
        linear = (vp[i] + vm[i + 1]) + 0.5 * (d[i - 1] - dm[i + 1]) + (2.0 / 3.0) * (h[i] + hm[i + 1])
        faces.append(linear + (fix_m - fix))
    return [faces[i + 1] - faces[i] for i in range(len(faces) - 1)]


def rounds(sizes):
    x, y, z = sizes
    return [(a, 0, 0) for a in range(1, x)], [(0, a, b) for a in range(y) for b in range(z)][1:]


def kernel(sizes, q_hbm, out_ref, px, py, pz, fx, fy, fz, tq, zsend, zleft, zright, ts0, ts1, tsa, tsb, speed_ref,
           gb, nb, tb, nxp, nyp, nzp, nzsend, nzleft, nzright, ay, tz,
           local_sem, send_sem, recv_sem, sa_sem, ra_sem, sb_sem, rb_sem):
    ngx, ngy, ngz = sizes
    X, Y, Z = px.shape[1] - 6, px.shape[2], px.shape[3]
    step = Z // SUB
    lines = X * Y
    ix, iy, iz = lax.axis_index("gx"), lax.axis_index("gy"), lax.axis_index("gz")
    offsets_a, offsets_b = rounds(sizes)

    load = pltpu.make_async_copy(q_hbm, px.at[:, 3 : 3 + X], local_sem)
    load.start()
    barrier = pltpu.get_barrier_semaphore()

    def peer_x(offset):
        return {"gx": lax.rem(ix + offset + ngx, ngx)}

    def peer_yz(a, b):
        return {"gy": lax.rem(iy + a + ngy, ngy), "gz": lax.rem(iz + b + ngz, ngz)}

    def peer(offset):
        return {**peer_x(offset[0]), **peer_yz(offset[1], offset[2])}

    for offset in offsets_a + offsets_b:
        pl.semaphore_signal(barrier, inc=1, device_id=peer(offset), device_id_type=MESH)

    row = lax.broadcasted_iota(jnp.int32, (SUB, LANES), 0)
    pxf = px.reshape(6 * (X + 6) * Y, LANES)
    tqf = tq.reshape(6 * Z, lines)
    halves = Y // SUB

    def rows_y(base, y):
        return pl.ds(base + y, SUB, stride=Y)

    def rows_z(base, b):
        return pl.ds(base + b, SUB, stride=step)

    load.wait()
    best = None
    for x in range(X):
        for half in range(halves):
            q = [px[c, 3 + x, half * SUB : (half + 1) * SUB, :] for c in range(6)]
            inverse, u, p = primitives(q)
            top = jnp.maximum(jnp.maximum(jnp.abs(u[0]), jnp.abs(u[1])), jnp.abs(u[2]))
            top = top + jnp.sqrt(gamma_gas * p * inverse)
            best = top if best is None else jnp.maximum(best, top)
    ts0[...] = jnp.max(best, axis=0, keepdims=True)
    pl.semaphore_wait(barrier, len(offsets_a) + len(offsets_b))

    def remote(source, target, index, peer, sends=send_sem, recvs=recv_sem):
        copy = pltpu.make_async_remote_copy(
            src_ref=source, dst_ref=target, send_sem=sends.at[index], recv_sem=recvs.at[index],
            device_id=peer, device_id_type=MESH,
        )
        copy.start()
        return copy

    reduce_a = [remote(ts0, tsa.at[o], o, peer(offset), sa_sem, ra_sem) for o, offset in enumerate(offsets_a)]
    xlow, xhigh, ilow, ihigh = pl.ds(0, 3), pl.ds(3 + X, 3), pl.ds(3, 3), pl.ds(X, 3)
    first, rest = pl.ds(0, 2), pl.ds(2, 4)
    halo_x0 = [
        remote(px.at[first, ihigh], px.at[first, xlow], 0, peer_x(1)),
        remote(px.at[first, ilow], px.at[first, xhigh], 1, peer_x(-1)),
    ]
    halo_x1 = [
        remote(px.at[rest, ihigh], px.at[rest, xlow], 6, peer_x(1)),
        remote(px.at[rest, ilow], px.at[rest, xhigh], 7, peer_x(-1)),
    ]

    def lay_out_y(c, carry):
        for y in range(Y):
            py[c, 3 + y] = pxf[rows_y((c * (X + 6) + 3) * Y, y), :]
        return carry

    lax.fori_loop(0, 6, lay_out_y, 0)
    halo_y = [
        remote(py.at[:, pl.ds(Y, 3)], py.at[:, pl.ds(0, 3)], 4, peer_yz(1, 0)),
        remote(py.at[:, pl.ds(3, 3)], py.at[:, pl.ds(3 + Y, 3)], 5, peer_yz(-1, 0)),
    ]

    def lay_out_z(c, carry):
        turned = px[c, 3 : 3 + X].reshape(lines, Z).T
        tq[c] = turned
        zsend[c] = jnp.where(row < 4, turned[:SUB], turned[Z - SUB :])
        return carry

    lax.fori_loop(0, 6, lay_out_z, 0)
    halo_z = [remote(zsend, zleft, 2, peer_yz(0, 1))]
    if ngz > 2:
        halo_z.append(remote(zsend, zright, 3, peer_yz(0, -1)))
        from_right = zright
    else:
        from_right = zleft

    for copy in reduce_a:
        copy.wait_recv()
    ts1[...] = jnp.maximum(ts0[...], jnp.max(tsa[...], axis=0))
    reduce_b = [remote(ts1, tsb.at[o], o, peer(offset), sb_sem, rb_sem) for o, offset in enumerate(offsets_b)]

    def fill_z(c, carry):
        for b in range(step):
            pz[c, 3 + b] = tqf[rows_z(c * Z, b), :]
        return carry

    lax.fori_loop(0, 6, fill_z, 0)

    def flux_x(at):
        for half in range(halves):
            part = pl.ds(half * SUB, SUB)
            values = scaled_flux([px[c, at, part, :] for c in range(6)], 0)
            for c in range(6):
                fx[c, at, part, :] = values[c]

    def flux_of(padded, target, k, at):
        values = scaled_flux([padded[c, at] for c in range(6)], k)
        for c in range(6):
            target[c, at] = values[c]

    def inner_x(t, carry):
        flux_x(3 + 2 * t)
        flux_x(4 + 2 * t)
        return carry

    def inner_yz(t, carry):
        for extra in range(2):
            flux_of(py, fy, 1, 3 + 2 * t + extra)
            flux_of(pz, fz, 2, 3 + 2 * t + extra)
        return carry

    lax.fori_loop(0, X // 2, inner_x, 0)

    lax.fori_loop(0, Y // 2, inner_yz, 0)
    def colour(q0, q1):
        return q0 / (q0 + q1)

    central = 1.0 / (2.0 * spacing)
    for copy in halo_z:
        copy.wait_recv()

    def join_z(c, carry):
        for s in range(3):
            low = pltpu.roll(pz[c, step + s], 1, 0)
            left = jnp.broadcast_to(zleft[c, pl.ds(5 + s, 1), :], (SUB, LANES))
            pz[c, s] = jnp.where(row == 0, left, low)
            high = pltpu.roll(pz[c, 3 + s], SUB - 1, 0)
            right = jnp.broadcast_to(from_right[c, pl.ds(s, 1), :], (SUB, LANES))
            pz[c, 3 + step + s] = jnp.where(row == SUB - 1, right, high)
        return carry

    lax.fori_loop(0, 6, join_z, 0)
    colours = [colour(pz[0, 2 + b], pz[1, 2 + b]) for b in range(step + 2)]
    for b in range(step):
        tb[rows_z(0, b), :] = (colours[b + 2] - colours[b]) * central
    gb[2] = tb[...].T
    for s in range(3):
        flux_of(pz, fz, 2, s)
        flux_of(pz, fz, 2, 3 + step + s)

    for copy in halo_y:
        copy.wait_recv()
    colours = [colour(py[0, 2 + y], py[1, 2 + y]) for y in range(Y + 2)]
    gbf = gb.reshape(3 * lines, LANES)
    for y in range(Y):
        gbf[rows_y(lines, y), :] = (colours[y + 2] - colours[y]) * central

    for copy in halo_x0:
        copy.wait_recv()
    for half in range(halves):
        part = pl.ds(half * SUB, SUB)
        colours = [colour(px[0, 2 + x, part, :], px[1, 2 + x, part, :]) for x in range(X + 2)]
        for x in range(X):
            at = pl.ds(x * Y + half * SUB, SUB)
            g = [(colours[x + 2] - colours[x]) * central, gb[1, at, :], gb[2, at, :]]
            gb[0, at, :] = g[0]
            length = jnp.sqrt(g[0] * g[0] + g[1] * g[1] + g[2] * g[2])
            inverse = 1.0 / jnp.maximum(length, normal_floor)
            nxp[1 + x, part, :] = g[0] * inverse
            nb[0, at, :] = g[1] * inverse
            nb[1, at, :] = g[2] * inverse
    nbf = nb.reshape(2 * lines, LANES)
    tb[...] = nb[1].T
    nzsend[...] = jnp.where(row < 4, tb[:SUB, :], tb[Z - SUB :, :])
    for y in range(Y):
        nyp[1 + y] = nbf[rows_y(0, y), :]
    for b in range(step):
        nzp[1 + b] = tb[rows_z(0, b), :]
    normals = [
        remote(nxp.at[pl.ds(X, 1)], nxp.at[pl.ds(0, 1)], 8, peer_x(1)),
        remote(nxp.at[pl.ds(1, 1)], nxp.at[pl.ds(1 + X, 1)], 9, peer_x(-1)),
        remote(nyp.at[pl.ds(Y, 1)], nyp.at[pl.ds(0, 1)], 10, peer_yz(1, 0)),
        remote(nyp.at[pl.ds(1, 1)], nyp.at[pl.ds(1 + Y, 1)], 11, peer_yz(-1, 0)),
        remote(nzsend, nzleft, 12, peer_yz(0, 1)),
    ]
    if ngz > 2:
        normals.append(remote(nzsend, nzright, 13, peer_yz(0, -1)))
        normal_right = nzright
    else:
        normal_right = nzleft
    for s in range(3):
        flux_of(py, fy, 1, s)
        flux_of(py, fy, 1, 3 + Y + s)

    for copy in reduce_b:
        copy.wait_recv()
    best = jnp.max(jnp.maximum(ts1[...], jnp.max(tsb[...], axis=0)), axis=1, keepdims=True)
    speed_ref[...] = jnp.broadcast_to(best, (SUB, LANES))

    def sweep_z(c, carry):
        scaled = (0.5 * SCALE) * speed_ref[...]
        count = step + 6
        parts = weno_tendency([fz[c, s] for s in range(count)], [pz[c, s] * scaled for s in range(count)])
        tzf = tz.reshape(6 * Z, lines)
        for b in range(step):
            tzf[rows_z(c * Z, b), :] = parts[b]
        return carry

    def sweep_y(c, carry):
        scaled = (0.5 * SCALE) * speed_ref[...]
        count = Y + 6
        parts = weno_tendency([fy[c, s] for s in range(count)], [py[c, s] * scaled for s in range(count)])
        ayf = ay.reshape(6 * lines, LANES)
        for y in range(Y):
            ayf[rows_y(c * lines, y), :] = parts[y]
        return carry

    lax.fori_loop(0, 6, sweep_z, 0)
    lax.fori_loop(0, 6, sweep_y, 0)

    for copy in halo_x1:
        copy.wait_recv()
    for s in range(3):
        flux_x(s)
        flux_x(3 + X + s)

    def sweep_x(c, carry):
        top = speed_ref[...]
        scaled = (0.5 * SCALE) * top
        timestep = (courant * spacing) / (3.0 * top)
        slope = timestep * (-1.0 / (spacing * SCALE))
        count = X + 6
        back = tz[c].T
        for half in range(halves):
            part = pl.ds(half * SUB, SUB)
            state = [px[c, s, part, :] for s in range(count)]
            parts = weno_tendency([fx[c, s, part, :] for s in range(count)], [v * scaled for v in state])
            for x in range(X):
                start = x * Y + half * SUB
                at = pl.ds(start, SUB)
                change = parts[x] + ay[c, at, :] + back[start : start + SUB]
                out_ref[c, x, part, :] = state[3 + x] + slope * change
        return carry

    lax.fori_loop(0, 6, sweep_x, 0)

    for copy in normals:
        copy.wait_recv()
    left = jnp.broadcast_to(nzleft[pl.ds(SUB - 1, 1), :], (SUB, LANES))
    nzp[0] = jnp.where(row == 0, left, pltpu.roll(nzp[step], 1, 0))
    right = jnp.broadcast_to(normal_right[pl.ds(0, 1), :], (SUB, LANES))
    nzp[1 + step] = jnp.where(row == SUB - 1, right, pltpu.roll(nzp[1], SUB - 1, 0))
    for b in range(step):
        tb[rows_z(0, b), :] = nzp[b + 2] - nzp[b]
    nb[1] = tb[...].T
    for y in range(Y):
        nbf[rows_y(0, y), :] = nyp[y + 2] - nyp[y]
    timestep = (courant * spacing) / (3.0 * speed_ref[...])
    for x in range(X):
        for half in range(halves):
            part = pl.ds(half * SUB, SUB)
            at = pl.ds(x * Y + half * SUB, SUB)
            q = [px[c, 3 + x, part, :] for c in range(5)]
            inverse = 1.0 / (q[0] + q[1])
            along = (nxp[x + 2, part, :] - nxp[x, part, :]) + nb[0, at, :] + nb[1, at, :]
            pull = ((-tension * central) * along) * timestep
            force = [pull * gb[k, at, :] for k in range(3)]
            for k in range(3):
                out_ref[2 + k, x, part, :] += force[k]
            out_ref[5, x, part, :] += (force[0] * q[2] + force[1] * q[3] + force[2] * q[4]) * inverse

    for copies in (reduce_a, reduce_b, halo_x0, halo_x1, halo_y, halo_z, normals):
        for copy in copies:
            copy.wait_send()


def solution(mesh):
    sizes = tuple(mesh.shape[name] for name in ("gx", "gy", "gz"))
    count_a, count_b = (max(len(offsets), 1) for offsets in rounds(sizes))

    def per_device(q):
        _, X, Y, Z = q.shape
        step = Z // SUB
        lines = X * Y
        assert X == SUB and Y % SUB == 0 and Z == LANES and lines == LANES and min(sizes) > 1

        def vmem(*shape):
            return pltpu.VMEM(shape, F32)

        dma = pltpu.SemaphoreType.DMA
        return pl.pallas_call(
            functools.partial(kernel, sizes),
            name="section",
            out_shape=pltpu.VMEM(q.shape, F32),
            in_specs=[pl.BlockSpec(memory_space=pltpu.HBM)],
            out_specs=pl.BlockSpec(memory_space=pltpu.VMEM),
            scratch_shapes=[
                vmem(6, X + 6, Y, Z), vmem(6, Y + 6, X, Z), vmem(6, step + 6, SUB, lines),
                vmem(6, X + 6, Y, Z), vmem(6, Y + 6, X, Z), vmem(6, step + 6, SUB, lines),
                vmem(6, Z, lines), vmem(6, SUB, lines), vmem(6, SUB, lines), vmem(6, SUB, lines),
                vmem(1, LANES), vmem(1, LANES), vmem(count_a, 1, LANES), vmem(count_b, 1, LANES),
                vmem(SUB, LANES),
                vmem(3, lines, Z), vmem(2, lines, Z), vmem(Z, lines),
                vmem(X + 2, Y, Z), vmem(Y + 2, X, Z), vmem(step + 2, SUB, lines),
                vmem(SUB, lines), vmem(SUB, lines), vmem(SUB, lines),
                vmem(6, lines, Z), vmem(6, Z, lines),
                dma, dma((14,)), dma((14,)),
                dma((count_a,)), dma((count_a,)), dma((count_b,)), dma((count_b,)),
            ],
            compiler_params=pltpu.CompilerParams(collective_id=0, has_side_effects=True, vmem_limit_bytes=24 * 2**20),
        )(pltpu.with_memory_space_constraint(q, pltpu.HBM))

    placed = P(None, "gx", "gy", "gz")
    return jax.shard_map(per_device, mesh=mesh, in_specs=(placed,), out_specs=placed, check_vma=False)
```

```python
import functools

import jax
import jax.numpy as jnp
from jax import lax
from jax.experimental import pallas as pl
from jax.experimental.pallas import tpu as pltpu
from jax.sharding import PartitionSpec as P

gamma_gas = 1.4
tension = 16.0
courant = 0.5
spacing = 0.5
weno_eps = 1e-06
normal_floor = 0.25

MESH = pl.DeviceIdType.MESH
SUB, LANES = 8, 128
SCALE = 0.125
F32 = jnp.float32


def primitives(q):
    inverse = 1.0 / (q[0] + q[1])
    u = [q[2 + k] * inverse for k in range(3)]
    kinetic = 0.5 * (q[2] * u[0] + q[3] * u[1] + q[4] * u[2])
    return inverse, u, (gamma_gas - 1.0) * (q[5] - kinetic)


def scaled_flux(q, k):
    _, u, p = primitives(q)
    speed = (0.5 * SCALE) * u[k]
    out = [q[c] * speed for c in range(5)] + [(q[5] + p) * speed]
    out[2 + k] = out[2 + k] + (0.5 * SCALE) * p
    return out


def correction(q0, q1, q2, third_a, third_b):
    a = q1 * q2
    b = 3.0 * (q0 * q1)
    total = a + (b + 6.0 * (q0 * q2))
    return (a * third_a + b * third_b) / total


def differences(v):
    n = len(v)
    d = [v[i + 1] - v[i] for i in range(n - 1)]
    second, middle, up, down = [None], [None], [None], [None]
    for i in range(1, n - 1):
        bend = d[i] - d[i - 1]
        slope = d[i] + d[i - 1]
        bend_4 = 4.0 * bend
        square, cross = bend_4 * bend, bend_4 * slope
        e = (slope * slope + 4.0 * weno_eps * SCALE * SCALE) + (13.0 / 12.0) * square
        base = e + square
        above, below = base + cross, base - cross
        second.append(bend)
        middle.append(e * e)
        up.append(above * above)
        down.append(below * below)
    third = [None, None] + [second[i] - second[i - 1] for i in range(2, n - 1)]
    return d, second, third, middle, up, down


def weno_tendency(flux, state):
    n = len(flux)
    vp = [f + s for f, s in zip(flux, state)]
    vm = [f - s for f, s in zip(flux, state)]
    d, h, j, mid, up, down = differences(vp)
    dm, hm, jm, mid_m, up_m, down_m = differences(vm)
    faces = []
    for i in range(2, n - 3):
        fix = correction(up[i - 1], mid[i], down[i + 1], j[i], 0.5 * j[i + 1])
        fix_m = correction(down_m[i + 2], mid_m[i + 1], up_m[i], jm[i + 2], 0.5 * jm[i + 1])
        linear = 3.0 * (vp[i] + vm[i + 1]) + 1.5 * (d[i - 1] - dm[i + 1]) + (h[i] + hm[i + 1])
        faces.append(linear + (fix_m - fix))
    return [faces[i + 1] - faces[i] for i in range(len(faces) - 1)]


def rounds(sizes):
    x, y, z = sizes
    return [(a, 0, 0) for a in range(1, x)], [(0, a, b) for a in range(y) for b in range(z)][1:]


def kernel(sizes, q_hbm, out_ref, px, py, pz, fx, fy, fz, tq, zsend, zleft, zright, ts0, ts1, tsa, tsb, speed_ref,
           gb, nb, tb, nxp, nyp, nzp, nzsend, nzleft, nzright, ay, tz,
           local_sem, send_sem, recv_sem, sa_sem, ra_sem, sb_sem, rb_sem):
    ngx, ngy, ngz = sizes
    X, Y, Z = px.shape[1] - 6, px.shape[2], px.shape[3]
    step = Z // SUB
    lines = X * Y
    ix, iy, iz = lax.axis_index("gx"), lax.axis_index("gy"), lax.axis_index("gz")
    offsets_a, offsets_b = rounds(sizes)

    load = pltpu.make_async_copy(q_hbm, px.at[:, 3 : 3 + X], local_sem)
    load.start()
    barrier = pltpu.get_barrier_semaphore()

    def peer_x(offset):
        return {"gx": lax.rem(ix + offset + ngx, ngx)}

    def peer_yz(a, b):
        return {"gy": lax.rem(iy + a + ngy, ngy), "gz": lax.rem(iz + b + ngz, ngz)}

    def peer(offset):
        return {**peer_x(offset[0]), **peer_yz(offset[1], offset[2])}

    for offset in offsets_a + offsets_b:
        pl.semaphore_signal(barrier, inc=1, device_id=peer(offset), device_id_type=MESH)

    row = lax.broadcasted_iota(jnp.int32, (SUB, LANES), 0)
    pxf = px.reshape(6 * (X + 6) * Y, LANES)
    tqf = tq.reshape(6 * Z, lines)
    halves = Y // SUB

    def rows_y(base, y):
        return pl.ds(base + y, SUB, stride=Y)

    def rows_z(base, b):
        return pl.ds(base + b, SUB, stride=step)

    load.wait()
    best = None
    for x in range(X):
        for half in range(halves):
            q = [px[c, 3 + x, half * SUB : (half + 1) * SUB, :] for c in range(6)]
            inverse, u, p = primitives(q)
            top = jnp.maximum(jnp.maximum(jnp.abs(u[0]), jnp.abs(u[1])), jnp.abs(u[2]))
            top = top + jnp.sqrt(gamma_gas * p * inverse)
            best = top if best is None else jnp.maximum(best, top)
    ts0[...] = jnp.max(best, axis=0, keepdims=True)
    pl.semaphore_wait(barrier, len(offsets_a) + len(offsets_b))

    def remote(source, target, index, peer, sends=send_sem, recvs=recv_sem):
        copy = pltpu.make_async_remote_copy(
            src_ref=source, dst_ref=target, send_sem=sends.at[index], recv_sem=recvs.at[index],
            device_id=peer, device_id_type=MESH,
        )
        copy.start()
        return copy

    reduce_a = [remote(ts0, tsa.at[o], o, peer(offset), sa_sem, ra_sem) for o, offset in enumerate(offsets_a)]
    xlow, xhigh, ilow, ihigh = pl.ds(0, 3), pl.ds(3 + X, 3), pl.ds(3, 3), pl.ds(X, 3)
    first, rest = pl.ds(0, 2), pl.ds(2, 4)
    halo_x0 = [
        remote(px.at[first, ihigh], px.at[first, xlow], 0, peer_x(1)),
        remote(px.at[first, ilow], px.at[first, xhigh], 1, peer_x(-1)),
    ]

    def lay_out_y(c, carry):
        for y in range(Y):
            py[c, 3 + y] = pxf[rows_y((c * (X + 6) + 3) * Y, y), :]
        return carry

    lax.fori_loop(0, 6, lay_out_y, 0)
    halo_y = [
        remote(py.at[:, pl.ds(Y, 3)], py.at[:, pl.ds(0, 3)], 4, peer_yz(1, 0)),
        remote(py.at[:, pl.ds(3, 3)], py.at[:, pl.ds(3 + Y, 3)], 5, peer_yz(-1, 0)),
    ]

    def lay_out_z(c, carry):
        turned = px[c, 3 : 3 + X].reshape(lines, Z).T
        tq[c] = turned
        zsend[c] = jnp.where(row < 4, turned[:SUB], turned[Z - SUB :])
        return carry

    lax.fori_loop(0, 6, lay_out_z, 0)
    halo_z = [remote(zsend, zleft, 2, peer_yz(0, 1))]
    if ngz > 2:
        halo_z.append(remote(zsend, zright, 3, peer_yz(0, -1)))
        from_right = zright
    else:
        from_right = zleft

    for copy in reduce_a:
        copy.wait_recv()
    ts1[...] = jnp.maximum(ts0[...], jnp.max(tsa[...], axis=0))
    reduce_b = [remote(ts1, tsb.at[o], o, peer(offset), sb_sem, rb_sem) for o, offset in enumerate(offsets_b)]

    halo_x1 = [
        remote(px.at[rest, ihigh], px.at[rest, xlow], 6, peer_x(1)),
        remote(px.at[rest, ilow], px.at[rest, xhigh], 7, peer_x(-1)),
    ]

    def fill_z(c, carry):
        for b in range(step):
            pz[c, 3 + b] = tqf[rows_z(c * Z, b), :]
        return carry

    lax.fori_loop(0, 6, fill_z, 0)

    def flux_x(at):
        for half in range(halves):
            part = pl.ds(half * SUB, SUB)
            values = scaled_flux([px[c, at, part, :] for c in range(6)], 0)
            for c in range(6):
                fx[c, at, part, :] = values[c]

    def flux_of(padded, target, k, at):
        values = scaled_flux([padded[c, at] for c in range(6)], k)
        for c in range(6):
            target[c, at] = values[c]

    def inner_x(t, carry):
        flux_x(3 + 2 * t)
        flux_x(4 + 2 * t)
        return carry

    def inner_yz(t, carry):
        for extra in range(2):
            flux_of(py, fy, 1, 3 + 2 * t + extra)
            flux_of(pz, fz, 2, 3 + 2 * t + extra)
        return carry

    lax.fori_loop(0, X // 2, inner_x, 0)

    lax.fori_loop(0, Y // 2, inner_yz, 0)
    def colour(q0, q1):
        return q0 / (q0 + q1)

    central = 1.0 / (2.0 * spacing)
    for copy in halo_z:
        copy.wait_recv()

    def join_z(c, carry):
        for s in range(3):
            low = pltpu.roll(pz[c, step + s], 1, 0)
            left = jnp.broadcast_to(zleft[c, pl.ds(5 + s, 1), :], (SUB, LANES))
            pz[c, s] = jnp.where(row == 0, left, low)
            high = pltpu.roll(pz[c, 3 + s], SUB - 1, 0)
            right = jnp.broadcast_to(from_right[c, pl.ds(s, 1), :], (SUB, LANES))
            pz[c, 3 + step + s] = jnp.where(row == SUB - 1, right, high)
        return carry

    lax.fori_loop(0, 6, join_z, 0)
    colours = [colour(pz[0, 2 + b], pz[1, 2 + b]) for b in range(step + 2)]
    for b in range(step):
        tb[rows_z(0, b), :] = (colours[b + 2] - colours[b]) * central
    gb[2] = tb[...].T
    for s in range(3):
        flux_of(pz, fz, 2, s)
        flux_of(pz, fz, 2, 3 + step + s)

    for copy in halo_y:
        copy.wait_recv()
    colours = [colour(py[0, 2 + y], py[1, 2 + y]) for y in range(Y + 2)]
    gbf = gb.reshape(3 * lines, LANES)
    for y in range(Y):
        gbf[rows_y(lines, y), :] = (colours[y + 2] - colours[y]) * central

    for copy in halo_x0:
        copy.wait_recv()
    for half in range(halves):
        part = pl.ds(half * SUB, SUB)
        colours = [colour(px[0, 2 + x, part, :], px[1, 2 + x, part, :]) for x in range(X + 2)]
        for x in range(X):
            at = pl.ds(x * Y + half * SUB, SUB)
            g = [(colours[x + 2] - colours[x]) * central, gb[1, at, :], gb[2, at, :]]
            gb[0, at, :] = g[0]
            length = jnp.sqrt(g[0] * g[0] + g[1] * g[1] + g[2] * g[2])
            inverse = 1.0 / jnp.maximum(length, normal_floor)
            nxp[1 + x, part, :] = g[0] * inverse
            nb[0, at, :] = g[1] * inverse
            nb[1, at, :] = g[2] * inverse
    nbf = nb.reshape(2 * lines, LANES)
    tb[...] = nb[1].T
    nzsend[...] = jnp.where(row < 4, tb[:SUB, :], tb[Z - SUB :, :])
    for y in range(Y):
        nyp[1 + y] = nbf[rows_y(0, y), :]
    for b in range(step):
        nzp[1 + b] = tb[rows_z(0, b), :]
    normals = [
        remote(nxp.at[pl.ds(X, 1)], nxp.at[pl.ds(0, 1)], 8, peer_x(1)),
        remote(nxp.at[pl.ds(1, 1)], nxp.at[pl.ds(1 + X, 1)], 9, peer_x(-1)),
        remote(nyp.at[pl.ds(Y, 1)], nyp.at[pl.ds(0, 1)], 10, peer_yz(1, 0)),
        remote(nyp.at[pl.ds(1, 1)], nyp.at[pl.ds(1 + Y, 1)], 11, peer_yz(-1, 0)),
        remote(nzsend, nzleft, 12, peer_yz(0, 1)),
    ]
    if ngz > 2:
        normals.append(remote(nzsend, nzright, 13, peer_yz(0, -1)))
        normal_right = nzright
    else:
        normal_right = nzleft
    for s in range(3):
        flux_of(py, fy, 1, s)
        flux_of(py, fy, 1, 3 + Y + s)

    for copy in reduce_b:
        copy.wait_recv()
    best = jnp.max(jnp.maximum(ts1[...], jnp.max(tsb[...], axis=0)), axis=1, keepdims=True)
    speed_ref[...] = jnp.broadcast_to(best, (SUB, LANES))

    def sweep_z(c, carry):
        scaled = (0.5 * SCALE) * speed_ref[...]
        count = step + 6
        parts = weno_tendency([fz[c, s] for s in range(count)], [pz[c, s] * scaled for s in range(count)])
        tzf = tz.reshape(6 * Z, lines)
        for b in range(step):
            tzf[rows_z(c * Z, b), :] = parts[b]
        return carry

    def sweep_y(c, carry):
        scaled = (0.5 * SCALE) * speed_ref[...]
        count = Y + 6
        parts = weno_tendency([fy[c, s] for s in range(count)], [py[c, s] * scaled for s in range(count)])
        ayf = ay.reshape(6 * lines, LANES)
        for y in range(Y):
            ayf[rows_y(c * lines, y), :] = parts[y]
        return carry

    lax.fori_loop(0, 6, sweep_z, 0)
    lax.fori_loop(0, 6, sweep_y, 0)

    for copy in halo_x1:
        copy.wait_recv()
    for s in range(3):
        flux_x(s)
        flux_x(3 + X + s)

    def sweep_x(c, carry):
        top = speed_ref[...]
        scaled = (0.5 * SCALE) * top
        timestep = (courant * spacing) / (3.0 * top)
        slope = timestep * (-1.0 / (3.0 * spacing * SCALE))
        count = X + 6
        back = tz[c].T
        for half in range(halves):
            part = pl.ds(half * SUB, SUB)
            state = [px[c, s, part, :] for s in range(count)]
            parts = weno_tendency([fx[c, s, part, :] for s in range(count)], [v * scaled for v in state])
            for x in range(X):
                start = x * Y + half * SUB
                at = pl.ds(start, SUB)
                change = parts[x] + ay[c, at, :] + back[start : start + SUB]
                out_ref[c, x, part, :] = state[3 + x] + slope * change
        return carry

    lax.fori_loop(0, 6, sweep_x, 0)

    for copy in normals:
        copy.wait_recv()
    left = jnp.broadcast_to(nzleft[pl.ds(SUB - 1, 1), :], (SUB, LANES))
    nzp[0] = jnp.where(row == 0, left, pltpu.roll(nzp[step], 1, 0))
    right = jnp.broadcast_to(normal_right[pl.ds(0, 1), :], (SUB, LANES))
    nzp[1 + step] = jnp.where(row == SUB - 1, right, pltpu.roll(nzp[1], SUB - 1, 0))
    for b in range(step):
        tb[rows_z(0, b), :] = nzp[b + 2] - nzp[b]
    nb[1] = tb[...].T
    for y in range(Y):
        nbf[rows_y(0, y), :] = nyp[y + 2] - nyp[y]
    timestep = (courant * spacing) / (3.0 * speed_ref[...])
    for x in range(X):
        for half in range(halves):
            part = pl.ds(half * SUB, SUB)
            at = pl.ds(x * Y + half * SUB, SUB)
            q = [px[c, 3 + x, part, :] for c in range(5)]
            inverse = 1.0 / (q[0] + q[1])
            along = (nxp[x + 2, part, :] - nxp[x, part, :]) + nb[0, at, :] + nb[1, at, :]
            pull = ((-tension * central) * along) * timestep
            force = [pull * gb[k, at, :] for k in range(3)]
            for k in range(3):
                out_ref[2 + k, x, part, :] += force[k]
            out_ref[5, x, part, :] += (force[0] * q[2] + force[1] * q[3] + force[2] * q[4]) * inverse

    for copies in (reduce_a, reduce_b, halo_x0, halo_x1, halo_y, halo_z, normals):
        for copy in copies:
            copy.wait_send()


def solution(mesh):
    sizes = tuple(mesh.shape[name] for name in ("gx", "gy", "gz"))
    count_a, count_b = (max(len(offsets), 1) for offsets in rounds(sizes))

    def per_device(q):
        _, X, Y, Z = q.shape
        step = Z // SUB
        lines = X * Y
        assert X == SUB and Y % SUB == 0 and Z == LANES and lines == LANES and min(sizes) > 1

        def vmem(*shape):
            return pltpu.VMEM(shape, F32)

        dma = pltpu.SemaphoreType.DMA
        return pl.pallas_call(
            functools.partial(kernel, sizes),
            name="section",
            out_shape=pltpu.VMEM(q.shape, F32),
            in_specs=[pl.BlockSpec(memory_space=pltpu.HBM)],
            out_specs=pl.BlockSpec(memory_space=pltpu.VMEM),
            scratch_shapes=[
                vmem(6, X + 6, Y, Z), vmem(6, Y + 6, X, Z), vmem(6, step + 6, SUB, lines),
                vmem(6, X + 6, Y, Z), vmem(6, Y + 6, X, Z), vmem(6, step + 6, SUB, lines),
                vmem(6, Z, lines), vmem(6, SUB, lines), vmem(6, SUB, lines), vmem(6, SUB, lines),
                vmem(1, LANES), vmem(1, LANES), vmem(count_a, 1, LANES), vmem(count_b, 1, LANES),
                vmem(SUB, LANES),
                vmem(3, lines, Z), vmem(2, lines, Z), vmem(Z, lines),
                vmem(X + 2, Y, Z), vmem(Y + 2, X, Z), vmem(step + 2, SUB, lines),
                vmem(SUB, lines), vmem(SUB, lines), vmem(SUB, lines),
                vmem(6, lines, Z), vmem(6, Z, lines),
                dma, dma((14,)), dma((14,)),
                dma((count_a,)), dma((count_a,)), dma((count_b,)), dma((count_b,)),
            ],
            compiler_params=pltpu.CompilerParams(collective_id=0, has_side_effects=True, vmem_limit_bytes=24 * 2**20),
        )(pltpu.with_memory_space_constraint(q, pltpu.HBM))

    placed = P(None, "gx", "gy", "gz")
    return jax.shard_map(per_device, mesh=mesh, in_specs=(placed,), out_specs=placed, check_vma=False)
```
